256 devices in a mesh: row: 32 (over y_lo, z, core), col: 8 (over x, y_hi).
Axes of the slice: x: 4, y: 4 (y_hi: 2, y_lo: 2; y = y_hi * 2 + y_lo), z: 8, core: 2. Of those that a mesh axis runs over, the one named last changes fastest.
Arguments:
- queries: bfloat16 [32768, 1024], P(('col', 'row')), may hold values from -150 to 150
- keys: bfloat16 [32768, 128], P(('row', 'col')), may hold values from -5 to 5
- values: bfloat16 [32768, 128], P(('row', 'col')), may hold values from -6 to 6
- segment_ids: int32 [32768], replicated, may hold values from 0 to 7, never falling along the last dimension, each value on 1 to 8192 neighbouring positions
Outputs:
- attended: bfloat16 [32768, 1024], P(('col', 'row'))
The draws below stay inside these ranges and needn't reach their ends.
All inputs are finite; a program needn't handle non-finite values.
Results may differ from the reference program's by a relative error of at most 0.013.
Values may be sent and summed in bfloat16 or wider, within the bound.
A program may use at most 128 MiB of HBM per device.

```python
import math
import jax
import jax.numpy as jnp
import numpy as np
from jax import lax

HQ = 8
HD = 128
TOK_DEV = 128
TOKENS = 32768


def paired_draw(key):
    key_rows = jnp.clip(jax.random.normal(jax.random.fold_in(key, 101), (TOKENS, HD), jnp.float32), -5.0, 5.0)
    query_rows = jnp.clip(jax.random.normal(jax.random.fold_in(key, 202), (TOKENS, HQ * HD), jnp.float32), -5.0, 5.0)
    return (query_rows, key_rows)


def draw_queries(key, part):
    return paired_draw(key)[0].astype(jnp.bfloat16)


def draw_keys(key, part):
    return paired_draw(key)[1].astype(jnp.bfloat16)


def levels(stream_key, dims, shards, smallest, high):
    def one(dim, shards_of):
        draws = jax.random.uniform(jax.random.fold_in(jax.random.fold_in(stream_key, 6), dim), (shards_of,), jnp.float32, smallest / len(shards), high / len(shards))
        return jnp.repeat(jnp.exp(draws), dims[dim] // shards_of).reshape((-1,) + (1,) * (len(dims) - dim - 1))

    loudness = one(*shards[0])
    for cut in shards[1:]:
        loudness = loudness * one(*cut)
    return loudness


def length_profile(number_of, total, most, skew):
    weights = [(1 << 20) // math.isqrt(rank ** skew) + 1 for rank in range(2, number_of + 1)]
    spare, counts = total - most - (number_of - 1), [1] * (number_of - 1)
    while spare > 0:
        candidates = [i for i in range(number_of - 1) if counts[i] < most]
        pool, left = sum([weights[i] for i in candidates]), spare
        for i in candidates:
            addition = min(most - counts[i], max(1, left * weights[i] // pool), spare)
            counts[i] = counts[i] + addition
            spare = spare - addition
    return np.array([most] + counts)


def uneven_parts(rng, number_of, total, limit, lean):
    if number_of == 2:
        one = jax.random.randint(rng, (), max(1, total - limit), min(limit, total - 1) + 1)
        return jnp.stack([one, total - one])
    sizes = jnp.asarray(length_profile(number_of, total, limit, lean), jnp.int32)
    twos = (number_of - 1) // 2
    giver, sink = sizes[1:1 + 2 * twos:2], sizes[2:2 + 2 * twos:2]
    room = jnp.minimum(giver - 1, limit - sink)
    shifted = jax.random.randint(jax.random.fold_in(rng, 1), (twos,), 0, 1 << 20) % (room + 1)
    sizes = sizes.at[1:1 + 2 * twos:2].set(giver - shifted).at[2:2 + 2 * twos:2].set(sink + shifted)
    return sizes[jax.random.permutation(jax.random.fold_in(rng, 2), number_of)]


def normal_values(key, dims, spread, reach, shards=(), held_as=jnp.bfloat16):
    level = levels(key, dims, shards, -0.22, 0.18) if shards else 1.0
    result = jax.random.normal(key, dims, jnp.float32) * spread * level
    return jnp.minimum(jnp.maximum(result, -reach), reach).astype(held_as)


def setup_inputs(seed: int = 0) -> dict:
    streams_of = jax.random.split(jax.random.key(seed), 5)
    return {
        "queries": draw_queries(jax.random.fold_in(streams_of[4], 71), 0),
        "keys": draw_keys(jax.random.fold_in(streams_of[4], 71), 0),
        "values": normal_values(streams_of[2], (TOKENS, HD), 1.0, 6.0, ((0, 256),)),
        "segment_ids": jnp.searchsorted(jnp.cumsum(uneven_parts(streams_of[3], 8, TOKENS, TOKENS // 4, 0)), jnp.arange(TOKENS), side="right").astype(jnp.int32),
    }


def reference(queries, keys, values, segment_ids):
    key_float = keys.astype(jnp.float32)
    value_float = values.astype(jnp.float32)
    block_rows = 2 * TOK_DEV
    block_count = TOKENS // block_rows
    key_pos = jnp.arange(TOKENS, dtype=jnp.int32)
    scale_factor = 1.0 / math.sqrt(HD)

    def attend_block(block_index):
        first_row = (block_index * block_rows).astype(jnp.int32)
        query_float = lax.dynamic_slice_in_dim(queries, first_row, block_rows, 0).astype(jnp.float32).reshape(block_rows, HQ, HD)
        query_seg = lax.dynamic_slice_in_dim(segment_ids, first_row, block_rows, 0)
        query_pos = first_row + jnp.arange(block_rows, dtype=jnp.int32)
        scores = jnp.einsum('qhd,kd->qhk', query_float, key_float, precision=lax.Precision.HIGHEST) * scale_factor
        visible = ((query_seg[:, None] == segment_ids[None, :]) & (key_pos[None, :] <= query_pos[:, None]))[:, None, :]
        row_max = lax.optimization_barrier(jnp.max(jnp.where(visible, scores, -1e+30), axis=2, keepdims=True))
        exp_terms = jnp.where(visible, jnp.exp(scores - row_max), 0.0)
        totals = lax.optimization_barrier(jnp.sum(exp_terms, axis=2))
        rounded = lax.optimization_barrier(exp_terms.astype(jnp.bfloat16))
        weights = rounded.astype(jnp.float32)
        numerator = jnp.einsum('qhk,kd->qhd', weights, value_float, precision=lax.Precision.HIGHEST)
        return (numerator / totals[..., None]).reshape(block_rows, HQ * HD).astype(jnp.bfloat16)
    attended = lax.map(attend_block, jnp.arange(block_count, dtype=jnp.int32))
    return attended.reshape(TOKENS, HQ * HD)
```

```python
import functools
import math

import jax
import jax.numpy as jnp
from jax import lax
from jax.experimental import pallas as pl
from jax.experimental.pallas import tpu as pltpu
from jax.sharding import PartitionSpec as P

HQ = 8
HD = 128
ROWS = 128
TILE = 512
GROUP = 256
NEG = -1e30
SCALE = math.log2(math.e) / math.sqrt(HD)


def attend_kernel(t0_ref, seg_ref, q_ref, kv_ref, o_ref, q_scr, kv_buf, m_scr, l_scr, acc_scr, sems):
    t0 = t0_ref[0]
    seg = seg_ref[...]
    starts = [jnp.sum(jnp.where(seg < s, 1.0, 0.0)).astype(jnp.int32) for s in range(1, HQ)]
    zero = jnp.int32(0)
    lo_first, lo_last = zero, zero
    for st in starts:
        lo_first = jnp.maximum(lo_first, jnp.where(st <= t0, st, zero))
        lo_last = jnp.maximum(lo_last, jnp.where(st <= t0 + ROWS - 1, st, zero))
    high = (t0 + ROWS - 1) // TILE
    low = lo_first // TILE
    count = high - low + 1

    def fetch(i):
        at = pl.multiple_of((high - i) * TILE, TILE)
        slot = lax.rem(i, 2)
        return pltpu.make_async_copy(kv_ref.at[pl.ds(at, TILE)], kv_buf.at[slot], sems.at[slot])

    fetch(0).start()
    for h in range(HQ):
        q_scr[h * ROWS : (h + 1) * ROWS, :] = q_ref[:, h * HD : (h + 1) * HD]
    m_scr[...] = jnp.full_like(m_scr, NEG)
    l_scr[...] = jnp.zeros_like(l_scr)
    acc_scr[...] = jnp.zeros_like(acc_scr)

    def tile(i, masked):
        slot = lax.rem(i, 2)
        base = (high - i) * TILE
        k = kv_buf[slot, :, :HD]
        v = kv_buf[slot, :, HD:]
        if masked:
            t = t0 + lax.broadcasted_iota(jnp.int32, (ROWS, TILE), 0)
            u = base + lax.broadcasted_iota(jnp.int32, (ROWS, TILE), 1)
            first = jnp.zeros_like(t)
            for st in starts:
                first = jnp.maximum(first, jnp.where(st <= t, st, 0))
            seen = (u <= t) & (u >= first)
            bias = jnp.where(seen, 0.0, NEG)
            bias = jnp.concatenate([bias] * (GROUP // ROWS), axis=0)
        for g in range(HQ * ROWS // GROUP):
            rows = slice(g * GROUP, (g + 1) * GROUP)
            s = lax.dot_general(
                q_scr[rows, :], k, (((1,), (1,)), ((), ())), preferred_element_type=jnp.float32
            )
            if masked:
                s = s + bias
            parts = [s[:, c : c + 128] for c in range(0, TILE, 128)]
            top = functools.reduce(jnp.maximum, parts)
            m_old = m_scr[rows, :]
            m_new = jnp.maximum(m_old, jnp.max(top, axis=1, keepdims=True))
            alpha = jnp.exp2((m_old - m_new) * SCALE)
            m_scr[rows, :] = m_new
            shift = m_new * SCALE
            terms = [jnp.exp2(x * SCALE - shift) for x in parts]
            l_scr[rows, :] = l_scr[rows, :] * alpha + functools.reduce(jnp.add, terms)
            weights = jnp.concatenate([x.astype(jnp.bfloat16) for x in terms], axis=1)
            acc_scr[rows, :] = acc_scr[rows, :] * alpha + jnp.dot(
                weights, v, preferred_element_type=jnp.float32
            )

    def step(i, carry):
        fetch(i).wait()

        @pl.when(i + 1 < count)
        def _():
            fetch(i + 1).start()

        base = (high - i) * TILE
        partial = (base + TILE > t0) | (base < lo_last)

        @pl.when(partial)
        def _():
            tile(i, True)

        @pl.when(jnp.logical_not(partial))
        def _():
            tile(i, False)

        return carry

    lax.fori_loop(0, count, step, 0)
    for h in range(HQ):
        rows = slice(h * ROWS, (h + 1) * ROWS)
        total = jnp.sum(l_scr[rows, :], axis=1, keepdims=True)
        o_ref[:, h * HD : (h + 1) * HD] = (acc_scr[rows, :] / total).astype(jnp.bfloat16)


def attend(t0, seg, queries, kv):
    stacked = HQ * ROWS
    return pl.pallas_call(
        attend_kernel,
        out_shape=jax.ShapeDtypeStruct(queries.shape, jnp.bfloat16),
        in_specs=[
            pl.BlockSpec(memory_space=pltpu.SMEM),
            pl.BlockSpec(memory_space=pltpu.VMEM),
            pl.BlockSpec(memory_space=pltpu.VMEM),
            pl.BlockSpec(memory_space=pl.ANY),
        ],
        out_specs=pl.BlockSpec(memory_space=pltpu.VMEM),
        scratch_shapes=[
            pltpu.VMEM((stacked, HD), jnp.bfloat16),
            pltpu.VMEM((2, TILE, 2 * HD), jnp.bfloat16),
            pltpu.VMEM((stacked, 128), jnp.float32),
            pltpu.VMEM((stacked, 128), jnp.float32),
            pltpu.VMEM((stacked, HD), jnp.float32),
            pltpu.SemaphoreType.DMA((2,)),
        ],
        name="attend",
    )(t0, seg, queries, kv)


def per_device(queries, keys, values, segment_ids):
    n_row = lax.axis_size("row")
    block = lax.axis_index("col") * n_row + lax.axis_index("row")
    t0 = (block * queries.shape[0]).astype(jnp.int32).reshape(1)
    kv = lax.all_gather(jnp.concatenate([keys, values], axis=1), ("row", "col"), axis=0, tiled=True)
    return attend(t0, segment_ids.reshape(-1, 128), queries, kv)


def solution(mesh):
    in_specs = (P(("col", "row"), None), P(("row", "col"), None), P(("row", "col"), None), P())
    out_specs = P(("col", "row"), None)
    return jax.shard_map(
        per_device, mesh=mesh, in_specs=in_specs, out_specs=out_specs, check_vma=False
    )
```

```python
import functools
import math

import jax
import jax.numpy as jnp
from jax import lax
from jax.experimental import pallas as pl
from jax.experimental.pallas import tpu as pltpu
from jax.sharding import PartitionSpec as P

HQ = 8
HD = 128
ROWS = 128
NZ = 8
NY = 4
GROUP = 256
NEG = -1e30
SCALE = math.log2(math.e) / math.sqrt(HD)
MESH = pl.DeviceIdType.MESH


def place():
    row, col = lax.axis_index("row"), lax.axis_index("col")
    core = lax.rem(row, 2)
    z = lax.rem(lax.div(row, 2), NZ)
    y = lax.rem(col, 2) * 2 + lax.div(row, 2 * NZ)
    x = lax.div(col, 2)
    return row, col, x, y, z, core


def exchange_kernel(
    k_ref, v_ref, win, p0_send, p0_recv, z_send, y_send, d_send, own_recv, pair_recv
):
    row, col, x, y, z, core = place()

    def device(yy, zz, cc):
        return (lax.rem(yy, 2) * NZ + zz) * 2 + cc, x * 2 + lax.div(yy, 2)

    held = row * 8 + col
    to_row = lax.rem(held, 32)
    to_z, to_core = lax.rem(lax.div(to_row, 2), NZ), lax.rem(to_row, 2)

    def first(i, target):
        zz, cc = (to_z, to_core) if target else (z, core)
        to_col = lax.rem(lax.div(held, 32) + i, 8)
        same = (to_row == row) & (to_col == col)
        out = []
        for n, ref in enumerate((k_ref, v_ref)):
            spot = win.at[2 * i, zz, cc, n]
            far = pltpu.make_async_remote_copy(
                ref, spot, p0_send.at[i, n], p0_recv.at[i, n], (to_row, to_col), MESH
            )
            near = pltpu.make_async_copy(ref, spot, p0_recv.at[i, n])
            out.append((far, near))
        return same, out

    def ring(d, zb, way, hop):
        to = lax.rem(z + (1 if way == 0 else NZ - 1), NZ)
        spot = win.at[d, zb, core]
        return pltpu.make_async_remote_copy(
            spot, spot, z_send.at[d // 2, way, hop], own_recv.at[d, zb], device(y, to, core), MESH
        )

    def across(d, zb, way):
        to = lax.rem(y + (1 if way == 0 else NY - 1), NY)
        return pltpu.make_async_remote_copy(
            win.at[d, zb, core],
            win.at[1 if way == 0 else 3, zb, core],
            y_send.at[way, zb],
            own_recv.at[1 if way == 0 else 3, zb],
            device(to, z, core),
            MESH,
        )

    def share(d, zb, mine):
        spot = win.at[d, zb, core if mine else 1 - core]
        return pltpu.make_async_remote_copy(
            spot, spot, d_send.at[d, zb], pair_recv.at[d, zb], device(y, z, 1 - core), MESH
        )

    def arrived(d, zb):
        spot = win.at[d, zb, core]
        pltpu.make_async_remote_copy(
            spot, spot, z_send.at[0, 0, 0], own_recv.at[d, zb], device(y, z, 1 - core), MESH
        ).wait_recv()

    def needed(d, zb):
        return zb <= z if d == 0 else zb >= z if d == 4 else None

    def maybe(cond, act):
        if cond is None:
            act()
        else:
            pl.when(cond)(act)

    def have(d, zb):
        if d == 0:
            pl.when(y < 3)(lambda: across(0, zb, 0).start())
            pl.when(y == 0)(lambda: across(0, zb, 1).start())
        if d == 4:
            pl.when(y == 3)(lambda: across(4, zb, 0).start())
            pl.when(y > 0)(lambda: across(4, zb, 1).start())
        maybe(needed(d, zb), lambda: share(d, zb, True).start())

    for i in (0, 2, 1):
        same, copies = first(i, True)
        for far, near in copies:
            pl.when(same)(lambda near=near: near.start())
            pl.when(jnp.logical_not(same))(lambda far=far: far.start())
    even = [lax.rem(core + e, 2) == 0 for e in range(3)]
    odd = [jnp.logical_not(e) for e in even]
    for i in (0, 2, 1):
        same, copies = first(i, False)
        for far, near in copies:
            pl.when(same)(lambda near=near: near.wait())
            pl.when(jnp.logical_not(same))(lambda far=far: far.wait_recv())
        ring(2 * i, z, 0, 0).start()
        ring(2 * i, z, 1, 0).start()
        have(2 * i, z)

    def later(zb):
        for d in (1, 3):
            arrived(d, zb)
            share(d, zb, True).start()

    for hop in range(1, 4):
        up, down = lax.rem(z + NZ - hop, NZ), lax.rem(z + hop, NZ)
        for i in (0, 2, 1):
            d = 2 * i
            arrived(d, up)
            maybe(None if hop < 3 else even[i], lambda: ring(d, up, 0, hop).start())
            have(d, up)
            arrived(d, down)
            maybe(None if hop < 3 else odd[i], lambda: ring(d, down, 1, hop).start())
            have(d, down)
        if hop == 1:
            later(z)
        else:
            later(lax.rem(z + NZ - hop + 1, NZ))
            later(lax.rem(z + hop - 1, NZ))
    last = lax.rem(z + 4, NZ)
    for i in (0, 2, 1):
        arrived(2 * i, last)
        have(2 * i, last)
    later(lax.rem(z + 5, NZ))
    later(lax.rem(z + 3, NZ))
    later(last)

    for d in range(5):
        for s in range(NZ):
            zb = lax.rem(z + s, NZ)
            maybe(needed(d, zb), lambda: share(d, zb, False).wait_recv())
            maybe(needed(d, zb), lambda: share(d, zb, True).wait_send())
    for i in range(3):
        same, copies = first(i, True)
        for far, near in copies:
            pl.when(jnp.logical_not(same))(lambda far=far: far.wait_send())
        for hop in range(4):
            up, down = lax.rem(z + NZ - hop, NZ), lax.rem(z + hop, NZ)
            maybe(None if hop < 3 else even[i], lambda: ring(2 * i, up, 0, hop).wait_send())
            maybe(None if hop < 3 else odd[i], lambda: ring(2 * i, down, 1, hop).wait_send())
    for zb in range(NZ):
        across(0, zb, 0).wait_send()
        across(0, zb, 1).wait_send()


def exchange(keys, values):
    return pl.pallas_call(
        exchange_kernel,
        out_shape=jax.ShapeDtypeStruct((5, NZ, 2, 2, ROWS, HD), jnp.bfloat16),
        in_specs=[pl.BlockSpec(memory_space=pl.ANY)] * 2,
        out_specs=pl.BlockSpec(memory_space=pltpu.VMEM),
        scratch_shapes=[
            pltpu.SemaphoreType.DMA((3, 2)),
            pltpu.SemaphoreType.DMA((3, 2)),
            pltpu.SemaphoreType.DMA((3, 2, 4)),
            pltpu.SemaphoreType.DMA((2, NZ)),
            pltpu.SemaphoreType.DMA((5, NZ)),
            pltpu.SemaphoreType.DMA((5, NZ)),
            pltpu.SemaphoreType.DMA((5, NZ)),
        ],
        compiler_params=pltpu.CompilerParams(has_side_effects=True),
        name="exchange",
    )(keys, values)


def attend_kernel(seg_ref, q_ref, win, o_ref, q_scr, m_scr, l_scr, acc_scr):
    row, col, x, y, z, core = place()
    t0 = (col * 32 + row) * ROWS
    band = (4 * x + y) * 16
    seg = seg_ref[...]
    starts = [jnp.sum(jnp.where(seg < s, 1.0, 0.0)).astype(jnp.int32) for s in range(1, HQ)]
    zero = jnp.int32(0)
    lo_first, lo_last = zero, zero
    for st in starts:
        lo_first = jnp.maximum(lo_first, jnp.where(st <= t0, st, zero))
        lo_last = jnp.maximum(lo_last, jnp.where(st <= t0 + ROWS - 1, st, zero))

    for h in range(HQ):
        q_scr[h * ROWS : (h + 1) * ROWS, :] = q_ref[:, h * HD : (h + 1) * HD]
    m_scr[...] = jnp.full_like(m_scr, NEG)
    l_scr[...] = jnp.zeros_like(l_scr)
    acc_scr[...] = jnp.zeros_like(acc_scr)

    def tile(pairs, masked):
        blocks = [(d, zb, cc) for d, zb in pairs for cc in (0, 1)]
        k = jnp.concatenate([win[d, zb, cc, 0] for d, zb, cc in blocks], axis=0)
        v = jnp.concatenate([win[d, zb, cc, 1] for d, zb, cc in blocks], axis=0)
        if masked:
            t = t0 + lax.broadcasted_iota(jnp.int32, (ROWS, 128), 0)
            lane = lax.broadcasted_iota(jnp.int32, (ROWS, 128), 1)
            start = jnp.zeros_like(t)
            for st in starts:
                start = jnp.maximum(start, jnp.where(st <= t, st, 0))
            biases = []
            for d, zb, cc in blocks:
                u = lane + (band - 16 * d + 2 * zb + cc) * ROWS
                bias = jnp.where((u <= t) & (u >= start), 0.0, NEG)
                biases.append(jnp.concatenate([bias] * (GROUP // ROWS), axis=0))
        for g in range(HQ * ROWS // GROUP):
            rows = slice(g * GROUP, (g + 1) * GROUP)
            s = lax.dot_general(
                q_scr[rows, :], k, (((1,), (1,)), ((), ())), preferred_element_type=jnp.float32
            )
            parts = [s[:, n * 128 : n * 128 + 128] for n in range(len(blocks))]
            if masked:
                parts = [p + b for p, b in zip(parts, biases)]
            top = functools.reduce(jnp.maximum, parts)
            m_old = m_scr[rows, :]
            m_new = jnp.maximum(m_old, jnp.max(top, axis=1, keepdims=True))
            alpha = jnp.exp2((m_old - m_new) * SCALE)
            m_scr[rows, :] = m_new
            shift = m_new * SCALE
            terms = [jnp.exp2(p * SCALE - shift) for p in parts]
            l_scr[rows, :] = l_scr[rows, :] * alpha + functools.reduce(jnp.add, terms)
            weights = jnp.concatenate([p.astype(jnp.bfloat16) for p in terms], axis=1)
            acc_scr[rows, :] = acc_scr[rows, :] * alpha + jnp.dot(
                weights, v, preferred_element_type=jnp.float32
            )

    tile([(0, z)], True)

    def step(i, carry):
        a = lax.rem(z + 2 * lax.rem(i, 4) + 1, NZ)
        b = lax.rem(a + 1, NZ)
        d = lax.div(i, 4)
        da = jnp.where(d > 0, d, jnp.where(a < z, 0, 4))
        db = jnp.where(d > 0, d, jnp.where(b < z, 0, 4))
        base_a = (band - 16 * da + 2 * a) * ROWS
        base_b = (band - 16 * db + 2 * b) * ROWS
        seen = (base_a + 256 > lo_first) | (base_b + 256 > lo_first)
        clear = (base_a >= lo_last) & (base_b >= lo_last)

        @pl.when(clear)
        def _():
            tile([(da, a), (db, b)], False)

        @pl.when(seen & jnp.logical_not(clear))
        def _():
            tile([(da, a), (db, b)], True)

        return carry

    lax.fori_loop(0, 16, step, 0)
    for h in range(HQ):
        rows = slice(h * ROWS, (h + 1) * ROWS)
        total = jnp.sum(l_scr[rows, :], axis=1, keepdims=True)
        o_ref[:, h * HD : (h + 1) * HD] = (acc_scr[rows, :] / total).astype(jnp.bfloat16)


def attend(seg, queries, window):
    stacked = HQ * ROWS
    return pl.pallas_call(
        attend_kernel,
        out_shape=jax.ShapeDtypeStruct(queries.shape, jnp.bfloat16),
        in_specs=[pl.BlockSpec(memory_space=pltpu.VMEM)] * 3,
        out_specs=pl.BlockSpec(memory_space=pltpu.VMEM),
        scratch_shapes=[
            pltpu.VMEM((stacked, HD), jnp.bfloat16),
            pltpu.VMEM((stacked, 128), jnp.float32),
            pltpu.VMEM((stacked, 128), jnp.float32),
            pltpu.VMEM((stacked, HD), jnp.float32),
        ],
        name="attend",
    )(seg, queries, window)


def per_device(queries, keys, values, segment_ids):
    return attend(segment_ids.reshape(-1, 128), queries, exchange(keys, values))


def solution(mesh):
    in_specs = (P(("col", "row"), None), P(("row", "col"), None), P(("row", "col"), None), P())
    out_specs = P(("col", "row"), None)
    return jax.shard_map(
        per_device, mesh=mesh, in_specs=in_specs, out_specs=out_specs, check_vma=False
    )
```

```python
import functools
import math

import jax
import jax.numpy as jnp
from jax import lax
from jax.experimental import pallas as pl
from jax.experimental.pallas import tpu as pltpu
from jax.sharding import PartitionSpec as P

HQ = 8
HD = 128
ROWS = 128
NX = 4
NY = 4
NZ = 8
GROUP = 256
STACK = HQ * ROWS
NEG = -1e30
SCALE = math.log2(math.e) / math.sqrt(HD)
MESH = pl.DeviceIdType.MESH


def fused_kernel(
    seg_ref, q_ref, k_ref, v_ref, o_ref,
    win, qt, ks, vs, m_scr, l_scr, acc,
    p_send, p_recv, z_send, x_send, r_send, y_send, d_send, own_recv, pair_recv,
):
    row, col = lax.axis_index("row"), lax.axis_index("col")
    core = lax.rem(row, 2)
    z = lax.rem(lax.div(row, 2), NZ)
    y = lax.rem(col, 2) * 2 + lax.div(row, 2 * NZ)
    x = lax.div(col, 2)
    held = row * 8 + col
    block = col * 32 + row

    def device(xx, yy, zz, cc):
        return (lax.rem(yy, 2) * NZ + zz) * 2 + cc, xx * 2 + lax.div(yy, 2)

    z_up, z_down = lax.rem(z + 1, NZ), lax.rem(z + NZ - 1, NZ)
    x_up, x_down = lax.rem(x + 1, NX), lax.rem(x + NX - 1, NX)
    y_up, y_down = lax.rem(y + 1, NY), lax.rem(y + NY - 1, NY)
    home = (lax.rem(held, 32), lax.div(held, 32))
    origin = (lax.div(block, 8), lax.rem(block, 8))
    same = held == block
    moved = jnp.logical_not(same)
    partner = device(x, y, z, 1 - core)
    y_far = lax.rem(y + 2, NY)
    ahead = device(jnp.where(y < 2, x, x_up), y_far, z, core)
    behind = device(jnp.where(y < 2, x_down, x), y_far, z, core)

    barrier = pltpu.get_barrier_semaphore()

    def greet(target):
        pl.semaphore_signal(barrier, 1, device_id=target, device_id_type=MESH)

    pl.when(moved)(lambda: greet(origin))
    greet(behind)
    greet(device(x_down, y, z, core))
    greet(device(x, y_up, z, core))
    greet(device(x, y_down, z, core))
    greet(device(x, y, z_up, core))
    greet(device(x, y, z_down, core))
    greet(partner)

    seg = seg_ref[...]
    starts = [
        jnp.sum(jnp.where(seg < s, 1.0, 0.0), keepdims=True).astype(jnp.int32) for s in range(1, HQ)
    ]
    far = jnp.full((1, 1), 1 << 20, jnp.int32)
    bounds = [jnp.zeros((1, 1), jnp.int32)] + starts + [far]
    lane = lax.broadcasted_iota(jnp.int32, (8, 128), 1)
    first = jnp.full((8, 128), -(1 << 20), jnp.int32)
    for s in range(HQ):
        first = jnp.where(lane == s, bounds[s], first)
    first = first[0:1, :]
    t_row = block * ROWS + lax.broadcasted_iota(jnp.int32, (16, 128), 1)
    which = lax.broadcasted_iota(jnp.int32, (16, 128), 0)
    mark = jnp.zeros((16, 128), jnp.float32)
    for s in range(HQ):
        inside = (t_row >= bounds[s]) & (t_row < bounds[s + 1]) & (which == s)
        mark = jnp.where(inside, 1.0, mark)
    mark = mark.astype(jnp.bfloat16)
    qt[HD:, :] = jnp.zeros((HD, STACK), jnp.bfloat16)
    for h in range(HQ):
        cols = slice(h * ROWS, (h + 1) * ROWS)
        qt[:HD, cols] = q_ref[:, h * HD : (h + 1) * HD].T
        qt[HD : HD + 16, cols] = mark
    m_scr[...] = jnp.full_like(m_scr, NEG)
    l_scr[...] = jnp.zeros_like(l_scr)
    acc[...] = jnp.zeros_like(acc)

    pl.semaphore_wait(barrier, 7 + moved.astype(jnp.int32))

    def remote(src, dst, send, recv, target):
        return pltpu.make_async_remote_copy(src, dst, send, recv, target, MESH)

    def initial(n, here):
        ref = (k_ref, v_ref)[n]
        zz, cc = (z, core) if here else (lax.rem(lax.div(home[0], 2), NZ), lax.rem(home[0], 2))
        return remote(ref, win.at[0, zz, cc, n], p_send.at[n], p_recv.at[n], home)

    def initial_near(n):
        return pltpu.make_async_copy((k_ref, v_ref)[n], win.at[0, z, core, n], p_recv.at[n])

    def ring(d, zb, way, hop):
        spot = win.at[d, zb, core]
        target = device(x, y, z_up if way == 0 else z_down, core)
        return remote(spot, spot, z_send.at[d // 2, way, hop], own_recv.at[d, zb], target)

    def over_x(zb):
        target = device(x_up, y, z, core)
        return remote(
            win.at[0, zb, core], win.at[4, zb, core], x_send.at[zb], own_recv.at[4, zb], target
        )

    def over_y(d, zb, way):
        to = 1 if way == 0 else 3
        target = device(x, y_up if way == 0 else y_down, z, core)
        return remote(
            win.at[d, zb, core], win.at[to, zb, core], y_send.at[way, zb], own_recv.at[to, zb], target
        )

    def skip_row():
        return remote(win.at[0, z, core], win.at[2, z, core], r_send, own_recv.at[2, z], ahead)

    def share(d, zb, mine):
        spot = win.at[d, zb, core if mine else 1 - core]
        return remote(spot, spot, d_send.at[d, zb], pair_recv.at[d, zb], partner)

    def arrived(d, zb):
        spot = win.at[d, zb, core]
        remote(spot, spot, d_send.at[d, zb], own_recv.at[d, zb], partner).wait_recv()

    def wanted(d, zb):
        return zb <= z if d == 0 else zb >= z if d == 4 else None

    def maybe(cond, act):
        if cond is None:
            act()
        else:
            pl.when(cond)(act)

    def give(d, zb):
        maybe(wanted(d, zb), lambda: share(d, zb, True).start())

    turn = [lax.rem(core + e, 2) == 0 for e in range(2)]

    def goes(e, way):
        return turn[e] if way == 0 else jnp.logical_not(turn[e])

    def at_hop(hop):
        up, down = lax.rem(z + NZ - hop, NZ), lax.rem(z + hop, NZ)
        return [(up, 0)] if hop == 4 else [(up, 0), (down, 1)]

    def onward(d, zb, way, hop):
        if hop < 3:
            ring(d, zb, way, hop).start()
        elif hop == 3:
            pl.when(goes(d // 2, way))(lambda: ring(d, zb, way, hop).start())

    def spread(zb):
        over_x(zb).start()
        pl.when(y < 3)(lambda: over_y(0, zb, 0).start())
        pl.when(y == 0)(lambda: over_y(0, zb, 1).start())
        give(0, zb)

    def current(hop):
        for zb, way in at_hop(hop):
            arrived(0, zb)
            onward(0, zb, way, hop)
            spread(zb)

    def skipped(hop):
        if hop == 0:
            arrived(2, z)
            ring(2, z, 0, 0).start()
            ring(2, z, 1, 0).start()
            give(2, z)
            return
        for zb, way in at_hop(hop):
            arrived(2, zb)
            onward(2, zb, way, hop)
            give(2, zb)

    def previous(hop):
        for zb, _ in at_hop(hop) if hop else [(z, 0)]:
            arrived(4, zb)
            pl.when(y == 3)(lambda: over_y(4, zb, 0).start())
            pl.when(y > 0)(lambda: over_y(4, zb, 1).start())
            give(4, zb)

    def beside(hop):
        for zb, _ in at_hop(hop) if hop else [(z, 0)]:
            for d in (1, 3):
                arrived(d, zb)
                give(d, zb)

    band = (NY * x + y) * 16
    sub = lax.broadcasted_iota(jnp.int32, (ROWS, 128), 0)

    def load(n, d, zb, cc):
        base = (band - 16 * d + 2 * zb + cc) * ROWS
        at = slice(n * ROWS, (n + 1) * ROWS)
        ks[at, :HD] = win[d, zb, cc, 0]
        ks[at, HD:] = jnp.where(sub + base < first, NEG, 0.0).astype(jnp.bfloat16)
        vs[:, at] = win[d, zb, cc, 1].T

    def absorb(keys, bias):
        def scores(g):
            return jnp.dot(
                ks[:keys, :], qt[:, g * GROUP : (g + 1) * GROUP], preferred_element_type=jnp.float32
            )

        groups = STACK // GROUP
        ready = scores(0)
        for g in range(groups):
            s = ready
            if g + 1 < groups:
                ready = scores(g + 1)
            if bias is not None:
                s = s + bias
            cols = slice(g * GROUP, (g + 1) * GROUP)
            m_old = m_scr[:, cols]
            m_new = jnp.maximum(m_old, jnp.max(s, axis=0, keepdims=True))
            m_scr[:, cols] = m_new
            alpha = jnp.exp2((m_old - m_new) * SCALE)
            terms = jnp.exp2(s * SCALE - m_new * SCALE)
            part = jnp.sum(terms.reshape(keys // 8, 8, GROUP), axis=0)
            l_scr[:, cols] = l_scr[:, cols] * alpha + part
            acc[:, cols] = acc[:, cols] * alpha + jnp.dot(
                vs[:, :keys], terms.astype(jnp.bfloat16), preferred_element_type=jnp.float32
            )

    for n in range(2):
        pl.when(same)(lambda n=n: initial_near(n).start())
        pl.when(moved)(lambda n=n: initial(n, False).start())
    for n in range(2):
        pl.when(same)(lambda n=n: initial_near(n).wait())
        pl.when(moved)(lambda n=n: initial(n, True).wait_recv())
    ring(0, z, 0, 0).start()
    ring(0, z, 1, 0).start()
    skip_row().start()
    spread(z)
    current(1)
    skipped(0)
    share(0, z, False).wait_recv()
    load(0, 0, z, 0)
    load(1, 0, z, 1)
    u = lax.broadcasted_iota(jnp.int32, (2 * ROWS, 128), 0)
    t = core * ROWS + lax.broadcasted_iota(jnp.int32, (2 * ROWS, 128), 1)
    causal = jnp.where(u <= t, 0.0, NEG)
    absorb(2 * ROWS, jnp.concatenate([causal] * (GROUP // ROWS), axis=1))
    previous(0)
    current(2)
    skipped(1)
    beside(0)

    def tile(e, carry):
        @pl.when(e == 1)
        def _():
            current(3)
            previous(1)
            skipped(2)

        @pl.when(e == 2)
        def _():
            beside(1)
            previous(2)

        @pl.when(e == 3)
        def _():
            current(4)
            skipped(3)

        @pl.when(e == 4)
        def _():
            beside(2)
            previous(3)

        @pl.when(e == 5)
        def _():
            skipped(4)
            previous(4)

        @pl.when(e == 6)
        def _():
            beside(3)

        @pl.when(e == 7)
        def _():
            beside(4)

        hop = lax.div(e + 1, 2)
        up, down = lax.rem(z + NZ - hop, NZ), lax.rem(z + hop, NZ)
        edge = (e == 0) | (e == 7)
        odd = lax.rem(e, 2) == 1

        def mix(zb):
            return jnp.where(zb < z, 0, 4)

        pairs = [
            (jnp.where(edge | odd, mix(up), 1), up),
            (jnp.where(edge | jnp.logical_not(odd), 1, mix(down)), down),
            (jnp.where(edge | odd, 2, 3), up),
            (jnp.where(edge | jnp.logical_not(odd), 3, 2), down),
        ]
        for n, (d, zb) in enumerate(pairs):
            share(d, zb, False).wait_recv()
            for cc in (0, 1):
                load(2 * n + cc, d, zb, cc)
        absorb(8 * ROWS, None)
        return carry

    lax.fori_loop(0, 8, tile, 0)

    for h in range(HQ):
        cols = slice(h * ROWS, (h + 1) * ROWS)
        total = jnp.sum(l_scr[:, cols], axis=0, keepdims=True)
        o_ref[:, h * HD : (h + 1) * HD] = (acc[:, cols] / total).T.astype(jnp.bfloat16)

    for n in range(2):
        pl.when(moved)(lambda n=n: initial(n, False).wait_send())
    skip_row().wait_send()
    for hop in range(4):
        for zb, way in at_hop(hop) if hop else [(z, 0), (z, 1)]:
            for d in (0, 2):
                if hop < 3:
                    ring(d, zb, way, hop).wait_send()
                else:
                    pl.when(goes(d // 2, way))(lambda d=d, zb=zb, way=way: ring(d, zb, way, 3).wait_send())
    for zb in range(NZ):
        over_x(zb).wait_send()
        over_y(0, zb, 0).wait_send()
        over_y(0, zb, 1).wait_send()
        for d in range(5):
            maybe(wanted(d, zb), lambda: share(d, zb, True).wait_send())


def per_device(queries, keys, values, segment_ids):
    return pl.pallas_call(
        fused_kernel,
        out_shape=jax.ShapeDtypeStruct(queries.shape, jnp.bfloat16),
        in_specs=[
            pl.BlockSpec(memory_space=pltpu.VMEM),
            pl.BlockSpec(memory_space=pltpu.VMEM),
            pl.BlockSpec(memory_space=pl.ANY),
            pl.BlockSpec(memory_space=pl.ANY),
        ],
        out_specs=pl.BlockSpec(memory_space=pltpu.VMEM),
        scratch_shapes=[
            pltpu.VMEM((5, NZ, 2, 2, ROWS, HD), jnp.bfloat16),
            pltpu.VMEM((2 * HD, STACK), jnp.bfloat16),
            pltpu.VMEM((8 * ROWS, 2 * HD), jnp.bfloat16),
            pltpu.VMEM((HD, 8 * ROWS), jnp.bfloat16),
            pltpu.VMEM((1, STACK), jnp.float32),
            pltpu.VMEM((8, STACK), jnp.float32),
            pltpu.VMEM((HD, STACK), jnp.float32),
            pltpu.SemaphoreType.DMA((2,)),
            pltpu.SemaphoreType.DMA((2,)),
            pltpu.SemaphoreType.DMA((2, 2, 4)),
            pltpu.SemaphoreType.DMA((NZ,)),
            pltpu.SemaphoreType.DMA,
            pltpu.SemaphoreType.DMA((2, NZ)),
            pltpu.SemaphoreType.DMA((5, NZ)),
            pltpu.SemaphoreType.DMA((5, NZ)),
            pltpu.SemaphoreType.DMA((5, NZ)),
        ],
        compiler_params=pltpu.CompilerParams(
            collective_id=1,
            has_side_effects=True,
        ),
        name="attend",
    )(segment_ids.reshape(-1, 128), queries, keys, values)


def solution(mesh):
    in_specs = (P(("col", "row"), None), P(("row", "col"), None), P(("row", "col"), None), P())
    out_specs = P(("col", "row"), None)
    return jax.shard_map(
        per_device, mesh=mesh, in_specs=in_specs, out_specs=out_specs, check_vma=False
    )
```
